256 devices in a mesh: dp: 8 (over x, core), param: 32 (over y, z).
Axes of the slice: x: 4, y: 4, z: 8, core: 2. Of those that a mesh axis runs over, the one named last changes fastest.
Arguments:
- train_grads: bfloat16 [7168, 212992], P('dp', 'param'), as said below
- query_grads: bfloat16 [256, 212992], P('dp', 'param'), as said below
Outputs:
- scores: float32 [256, 7168], P('param', 'dp')
Inputs may be any that keep to these rules, and one draw needn't show every extreme that they name: `train_grads`: finite real values. `query_grads`: finite real values.
All inputs are finite; a program needn't handle non-finite values.
Results may differ from the reference program's by a relative error of at most 0.0003.
Values may be sent and summed in bfloat16 or wider, within the bound.
A program may use at most 64 MiB of HBM per device.

```python
import math
import jax
import jax.numpy as jnp
from jax import lax

TR_DEV = 896
GRAD = 212992
NTR = 7168
NQ = 256
N_DP = 8


latent_count = 256


decay_power = 0.35


def shared_basis(key):
    base = jax.random.fold_in(key, 7)
    spread = jax.random.uniform(jax.random.fold_in(base, 1), (GRAD,), jnp.float32)
    column_scale = jnp.exp(math.log(10.0) * spread) * (1.0 + 2.0 * jnp.arange(GRAD, dtype=jnp.float32) / GRAD)
    basis = jax.random.normal(jax.random.fold_in(base, 2), (latent_count, GRAD), jnp.float32)
    return (column_scale, basis)


def make_grads(key, salt, row_count):
    column_scale, basis = shared_basis(key)
    inner = jax.random.fold_in(key, salt)
    decay = jnp.power(jnp.arange(latent_count, dtype=jnp.float32) + 1.0, -decay_power)
    decay = decay / jnp.sqrt(jnp.sum(decay * decay))
    weights = jax.random.normal(jax.random.fold_in(inner, 1), (row_count, latent_count), jnp.float32) * decay[None, :]
    noise = jax.random.normal(jax.random.fold_in(inner, 2), (row_count, GRAD), jnp.float32)
    spread = jax.random.uniform(jax.random.fold_in(inner, 3), (row_count,), jnp.float32)
    mixed = jnp.dot(weights, basis) + 0.5 * noise
    row_scale = jnp.exp(math.log(10.0) * spread)
    return (row_scale[:, None] * column_scale[None, :] * mixed).astype(jnp.bfloat16)


def draw_train_grads(key, part):
    return make_grads(key, 11, NTR)


def draw_query_grads(key, part):
    return make_grads(key, 13, NQ)


def setup_inputs(seed: int = 0) -> dict:
    splits = jax.random.split(jax.random.key(seed), 3)
    return {
        "train_grads": draw_train_grads(jax.random.fold_in(splits[2], 71), 0),
        "query_grads": draw_query_grads(jax.random.fold_in(splits[2], 71), 0),
    }


epsilon = 1e-06

def reference(train_grads, query_grads):
    query_norm = lax.optimization_barrier(jnp.sum(jnp.square(query_grads.astype(jnp.float32)), axis=1))
    blocks = train_grads.reshape(N_DP, TR_DEV, GRAD)

    def one_block(block):
        products = lax.dot_general(query_grads, block, (((1,), (1,)), ((), ())), preferred_element_type=jnp.float32)
        block_norm = lax.optimization_barrier(jnp.sum(jnp.square(block.astype(jnp.float32)), axis=1))
        return (products, block_norm)
    products, train_norm = lax.map(one_block, blocks)
    products = jnp.transpose(products, (1, 0, 2)).reshape(NQ, NTR)
    train_norm = train_norm.reshape(NTR)
    return products * lax.rsqrt(query_norm + epsilon)[:, None] * lax.rsqrt(train_norm + epsilon)[None, :]
```

```python
import jax
import jax.numpy as jnp
from jax import lax
from jax.experimental import pallas as pl
from jax.experimental.pallas import tpu as pltpu
from jax.sharding import PartitionSpec as P

epsilon = 1e-06

NX, NY, NZ, NDP = 4, 4, 8, 8
TRAIN, DEPTH = 896, 6656
HALF = 16
LANES = 128
WIDTHS = (2048, 2048, 1536, 1024)
CUTS = tuple((sum(WIDTHS[:i]), w) for i, w in enumerate(WIDTHS))
NK = len(CUTS)
FAR_FIRST = (4, 3, 5, 2, 6, 1, 7)
GROUPS = (
    ((0, 0), (0, 1), (1, 0), (1, 1), (2, 0), (3, 0), (4, 0), (5, 0)),
    ((2, 1), (3, 1), (4, 1), (5, 1)),
    ((6, 0), (6, 1), (7, 0), (7, 1)),
)


def dot_rows(a, b):
    return lax.dot_general(a, b, (((1,), (1,)), ((), ())), preferred_element_type=jnp.float32)


def row_sums(lanes):
    high = lanes.astype(jnp.bfloat16)
    rest = lanes - high.astype(jnp.float32)
    mid = rest.astype(jnp.bfloat16)
    low = (rest - mid.astype(jnp.float32)).astype(jnp.bfloat16)
    ones = jnp.ones((16, 2 * LANES), jnp.bfloat16)
    both = jnp.concatenate([high, mid], axis=1)
    return (dot_rows(ones, both) + dot_rows(ones[:, :LANES], low))[0:1, :]


def kernel(
    train, query, out,
    q, t, p, zin, zout, zsum, yin, tacc, qall, norm, nz, nsum, ny, nall,
    q_sem, t_sem, out_sem, mate_sem, in_sem, pass_sem,
    z_send, z_recv, relay_recv, y_send, y_recv, qn_send, qn_recv, nz_send, nz_recv, ny_send, ny_recv,
):
    dp, param = lax.axis_index("dp"), lax.axis_index("param")
    x, c = dp // 2, dp % 2
    y, z = param // NZ, param % NZ
    right = (((x + 1) % NX) * 2 + c, param)
    left = (((x + NX - 1) % NX) * 2 + c, param)
    mate = (x * 2 + 1 - c, param)

    def at_z(d):
        return (dp, y * NZ + (z + d) % NZ)

    def at_y(d):
        return (dp, ((y + d) % NY) * NZ + z)

    def at_dp(d):
        return ((dp + d) % NDP, param)

    q_loads, t_loads = [], []
    for h in range(2):
        load = pltpu.make_async_copy(query.at[pl.ds(h * HALF, HALF), :], q.at[0, h], q_sem.at[h])
        load.start()
        q_loads.append(load)
    peers = [at_dp(d) for d in range(1, NDP)]
    peers += [at_z(d) for d in range(1, NZ)] + [at_y(d) for d in range(1, NY)]
    barrier = pltpu.get_barrier_semaphore()
    for peer in peers:
        pl.semaphore_signal(barrier, inc=1, device_id=peer, device_id_type=pl.DeviceIdType.MESH)

    def squares(ref_rows, k):
        total = jnp.zeros((HALF, LANES), jnp.float32)
        for j in range(CUTS[k][1] // LANES):
            v = ref_rows(pl.ds(CUTS[k][0] + j * LANES, LANES)).astype(jnp.float32)
            total = total + v * v
        return total

    for load in q_loads:
        load.wait()
    for i in range(TRAIN // LANES):
        rows = pl.ds(i * LANES, LANES)
        load = pltpu.make_async_copy(train.at[rows, :], t.at[rows, :], t_sem.at[i])
        load.start()
        t_loads.append(load)
    own = []
    for h in range(2):
        total = squares(lambda s, h=h: q[0, h, :, s], 0)
        for k in range(1, NK):
            total = total + squares(lambda s, h=h: q[0, h, :, s], k)
        own.append(total)
    own += [jnp.zeros((LANES - 2 * HALF, LANES), jnp.float32)]
    qall[dp] = row_sums(jnp.concatenate(own, axis=0))

    pl.semaphore_wait(barrier, len(peers))

    def remote(src, dst, send, recv, to):
        return pltpu.make_async_remote_copy(
            src_ref=src, dst_ref=dst, send_sem=send, recv_sem=recv, device_id=to,
            device_id_type=pl.DeviceIdType.MESH,
        )

    def await_in(like, sem):
        remote(like, like, sem, sem, mate).wait_recv()

    def await_out(like, sem):
        remote(like, like, sem, sem, mate).wait_send()

    def hop(src, dst, h, k, recv, to):
        k0, w = CUTS[k]
        piece = pl.ds(k0, w)
        remote(q.at[src, h, :, piece], q.at[dst, h, :, piece], out_sem, recv, to).start()

    for d in range(1, NDP):
        remote(qall.at[dp], qall.at[dp], qn_send, qn_recv, at_dp(d)).start()

    for h in range(2):
        for k in range(NK):
            hop(0, 2, h, k, in_sem.at[h, k], right)
            hop(0, 4, h, k, in_sem.at[h, k], left)
        remote(q.at[0, h], q.at[1, h], out_sem, mate_sem, mate).start()

    def products(g, first, last):
        k0, w = CUTS[first][0], sum(WIDTHS[first:last])
        a = jnp.concatenate([q[s, h, :, pl.ds(k0, w)] for s, h in GROUPS[g]], axis=0)
        part = dot_rows(a, t[:, pl.ds(k0, w)])
        for i, (s, h) in enumerate(GROUPS[g]):
            piece = part[i * HALF : (i + 1) * HALF].reshape(2, 8, TRAIN)
            where = pl.ds(4 * s + 2 * h, 2)
            p[where] = piece if first == 0 else p[where] + piece

    def block_of(r, zt):
        return 4 * (2 * r + (zt // 4 + c) % 2) + zt % 4

    def z_copy(src, dst, sem, d):
        remote(src, dst, z_send, sem, at_z(d)).start()

    def mine(r, d):
        return p.at[block_of(r, (z + d) % NZ)]

    def send_z(r):
        for d in FAR_FIRST:
            z_copy(mine(r, d), zin.at[r, d - 1], z_recv.at[r], d)

    PLUS, MINUS = pl.ds(0, 512), pl.ds(512, TRAIN - 512)

    def send_near(half, *groups):
        def each(d, go):
            for r in groups:
                if half is None:
                    go(r)
                else:
                    pl.when(((z + d) % NZ % 4) // 2 == half)(lambda r=r: go(r))

        def split(r):
            z_copy(mine(r, 4).at[:, PLUS], zin.at[r, 6, :, PLUS], relay_recv.at[r], 2)
            z_copy(mine(r, 4).at[:, MINUS], zin.at[r, 6, :, MINUS], relay_recv.at[r], 6)

        each(4, split)
        each(3, lambda r: z_copy(mine(r, 3), zin.at[r, 4], relay_recv.at[r], 1))
        each(5, lambda r: z_copy(mine(r, 5), zin.at[r, 5], relay_recv.at[r], 7))
        each(1, lambda r: z_copy(mine(r, 1), zin.at[r, 0], z_recv.at[r], 1))
        each(7, lambda r: z_copy(mine(r, 7), zin.at[r, 1], z_recv.at[r], 7))

    def relay(r):
        await_in(zin.at[r, pl.ds(4, 3)], relay_recv.at[r])
        for i, (d, part) in enumerate(((2, PLUS), (6, MINUS))):
            zout[r, i] = p[block_of(r, (z + d) % NZ)] + zin[r, 4 + i]
            zout[r, i, :, part] += zin[r, 6, :, part]
            z_copy(zout.at[r, i], zin.at[r, 2 + i], z_recv.at[r], d)

    home = [x, (x + NX - 1) % NX, (x + 1) % NX, (x + 2) % NX]

    def send_y(r):
        count = NZ - 1 if r == 3 else 4
        await_in(zin.at[r, pl.ds(0, count)], z_recv.at[r])
        total = p[block_of(r, z)]
        for i in range(count):
            total = total + zin[r, i]
        zsum[r] = total
        d = (home[r] + NY - y) % NY

        @pl.when(d != 0)
        def _():
            remote(zsum.at[r], yin.at[d - 1], y_send, y_recv, (dp, home[r] * NZ + z)).start()

    def arrive(g, k):
        k0, w = CUTS[k]
        await_in(q.at[2, :, :, pl.ds(k0, w)], in_sem.at[g, k])
        if g < 2:
            hop(2, 3, g, k, pass_sem.at[g, k], mate)
            hop(4, 5, g, k, pass_sem.at[g, k], mate)
            if g == 0:
                hop(2, 6, 0, k, in_sem.at[2, k], right)
            else:
                hop(4, 6, 1, k, in_sem.at[2, k], left)
        else:
            hop(6, 7, 0, k, pass_sem.at[2, k], mate)
            hop(6, 7, 1, k, pass_sem.at[2, k], mate)

    def multiply(g, first, last):
        if g == 0 and first == 0:
            await_in(q.at[1], mate_sem)
        for k in range(first, last):
            k0, w = CUTS[k]
            await_in(q.at[2, :, :, pl.ds(k0, w)], pass_sem.at[g, k])

        @pl.when(x >= 0)
        def _():
            products(g, first, last)

    def train_norms(first, last):
        def rows_of(i, carry):
            rows = pl.ds(pl.multiple_of(i * HALF, HALF), HALF)
            total = squares(lambda s: t[rows, s], 0)
            for k in range(1, NK):
                total = total + squares(lambda s, k=k: t[rows, s], k)
            tacc[rows, :] = total
            return carry

        for i in range(first, last):
            t_loads[i].wait()
            lax.fori_loop(i * LANES // HALF, (i + 1) * LANES // HALF, rows_of, 0)

    def send_norms():
        row = row_sums(tacc[...])
        await_in(qall.at[pl.ds(0, NDP - 1)], qn_recv)
        for i in range(NDP):
            norm[pl.ds(i, 1), :] = qall[i]
        for i in range(TRAIN // LANES):
            norm[pl.ds(NDP + i, 1), :] = row[:, i * LANES : (i + 1) * LANES]
        norm[pl.ds(15, 1), :] = jnp.zeros((1, LANES), jnp.float32)
        for d in FAR_FIRST:
            remote(norm, nz.at[d - 1], nz_send, nz_recv, at_z(d)).start()

    def add_norms():
        await_in(nz, nz_recv)
        total = norm[...]
        for d in range(NZ - 1):
            total = total + nz[d]
        nsum[...] = total
        for d in range(1, NY):
            remote(nsum, ny.at[d - 1], ny_send, ny_recv, at_y(d)).start()

    todo = [
        (train_norms, 0, 5),
        (arrive, 0, 0),
        (train_norms, 5, 7),
        (arrive, 0, 1),
        (arrive, 0, 2),
        (send_norms,),
        (arrive, 0, 3),
        (multiply, 0, 0, 2),
        (arrive, 1, 0),
        (arrive, 1, 1),
        (multiply, 0, 2, 4),
        (send_near, None, 0),
        (send_near, 0, 1, 2),
        (arrive, 1, 2),
        (arrive, 1, 3),
        (multiply, 1, 0, 2),
        (arrive, 2, 0),
        (multiply, 1, 2, 4),
        (relay, 0),
        (send_near, 1, 1, 2),
        (add_norms,),
        (arrive, 2, 1),
        (multiply, 2, 0, 1),
        (arrive, 2, 2),
        (multiply, 2, 1, 2),
        (arrive, 2, 3),
        (multiply, 2, 2, 3),
        (relay, 1),
        (relay, 2),
        (multiply, 2, 3, 4),
        (send_z, 3),
        (send_y, 0),
        (send_y, 1),
        (send_y, 2),
        (send_y, 3),
    ]
    for what, *how in todo:
        what(*how)

    await_in(ny, ny_recv)
    norms = nsum[...]
    for d in range(NY - 1):
        norms = norms + ny[d]
    nall[...] = norms
    train_norm = jnp.concatenate([norms[NDP + i : NDP + i + 1, :] for i in range(TRAIN // LANES)], axis=1)
    lane = lax.broadcasted_iota(jnp.int32, (8, LANES), 1)
    sub = lax.broadcasted_iota(jnp.int32, (8, LANES), 0)
    rows_norm = jnp.broadcast_to(nall[pl.ds(2 * y + z // 4, 1), :], (8, LANES))
    query_norm = jnp.sum(jnp.where(lane == sub + 8 * (z % 4), rows_norm, 0.0), axis=1, keepdims=True)
    query_scale = lax.rsqrt(query_norm + epsilon)
    train_scale = lax.rsqrt(train_norm + epsilon)

    ahead = (y + NX - x) % NX
    total = zsum[jnp.where(ahead == 0, 0, jnp.where(ahead == 3, 1, ahead + 1))]
    await_in(yin, y_recv)
    for d in range(NY - 1):
        total = total + yin[d]
    out[...] = total * query_scale * train_scale

    await_out(q.at[pl.ds(0, 7)], out_sem)
    await_out(zin, z_send)
    await_out(yin, y_send)
    await_out(qall.at[pl.ds(0, NDP - 1)], qn_send)
    await_out(nz, nz_send)
    await_out(ny, ny_send)


def per_device(train_grads, query_grads):
    f32, bf16 = jnp.float32, jnp.bfloat16
    dma = pltpu.SemaphoreType.DMA
    return pl.pallas_call(
        kernel,
        name="scores",
        out_shape=jax.ShapeDtypeStruct((8, TRAIN), f32),
        in_specs=[pl.BlockSpec(memory_space=pl.ANY)] * 2,
        out_specs=pl.BlockSpec(memory_space=pltpu.VMEM),
        scratch_shapes=[
            pltpu.VMEM((8, 2, HALF, DEPTH), bf16),
            pltpu.VMEM((TRAIN, DEPTH), bf16),
            pltpu.VMEM((32, 8, TRAIN), f32),
            pltpu.VMEM((4, NZ - 1, 8, TRAIN), f32),
            pltpu.VMEM((3, 2, 8, TRAIN), f32),
            pltpu.VMEM((4, 8, TRAIN), f32),
            pltpu.VMEM((NY - 1, 8, TRAIN), f32),
            pltpu.VMEM((TRAIN, LANES), f32),
            pltpu.VMEM((NDP, 1, LANES), f32),
            pltpu.VMEM((16, LANES), f32),
            pltpu.VMEM((NZ - 1, 16, LANES), f32),
            pltpu.VMEM((16, LANES), f32),
            pltpu.VMEM((NY - 1, 16, LANES), f32),
            pltpu.VMEM((16, LANES), f32),
            dma((2,)),
            dma((TRAIN // LANES,)),
            dma(()),
            dma(()),
            dma((3, NK)),
            dma((3, NK)),
            dma(()),
            dma((4,)),
            dma((3,)),
        ]
        + [dma(())] * 8,
        compiler_params=pltpu.CompilerParams(
            collective_id=0, has_side_effects=True, vmem_limit_bytes=66_700_000
        ),
    )(train_grads, query_grads)


def solution(mesh):
    return jax.shard_map(
        per_device,
        mesh=mesh,
        in_specs=(P("dp", "param"), P("dp", "param")),
        out_specs=P("param", "dp"),
        check_vma=False,
    )
```

```python
import jax
import jax.numpy as jnp
from jax import lax
from jax.experimental import pallas as pl
from jax.experimental.pallas import tpu as pltpu
from jax.sharding import PartitionSpec as P

epsilon = 1e-06

NX, NY, NZ, NDP = 4, 4, 8, 8
TRAIN, DEPTH = 896, 6656
HALF = 16
LANES = 128
WIDTHS = (2048, 2048, 1536, 1024)
CUTS = tuple((sum(WIDTHS[:i]), w) for i, w in enumerate(WIDTHS))
NK = len(CUTS)
FAR_FIRST = (4, 3, 5, 2, 6, 1, 7)
GROUPS = (
    ((0, 0), (0, 1), (1, 0), (1, 1)),
    tuple((s, h) for s in range(2, 6) for h in range(2)),
    ((6, 0), (6, 1), (7, 0), (7, 1)),
)


def dot_rows(a, b):
    return lax.dot_general(a, b, (((1,), (1,)), ((), ())), preferred_element_type=jnp.float32)


def row_sums(lanes):
    high = lanes.astype(jnp.bfloat16)
    rest = lanes - high.astype(jnp.float32)
    mid = rest.astype(jnp.bfloat16)
    low = (rest - mid.astype(jnp.float32)).astype(jnp.bfloat16)
    ones = jnp.ones((16, 2 * LANES), jnp.bfloat16)
    both = jnp.concatenate([high, mid], axis=1)
    return (dot_rows(ones, both) + dot_rows(ones[:, :LANES], low))[0:1, :]


def kernel(
    train, query, out,
    q, t, p, zin, zout, zsum, yin, tacc, qall, norm, nz, nsum, ny, nall,
    far_sem, q_sem, t_sem, out_sem, mate_sem, in_sem, pass_sem,
    z_send, z_recv, relay_recv, y_send, y_recv, qn_send, qn_recv, nz_send, nz_recv, ny_send, ny_recv,
):
    dp, param = lax.axis_index("dp"), lax.axis_index("param")
    x, c = dp // 2, dp % 2
    y, z = param // NZ, param % NZ
    right = (((x + 1) % NX) * 2 + c, param)
    left = (((x + NX - 1) % NX) * 2 + c, param)
    mate = (x * 2 + 1 - c, param)

    def at_z(d):
        return (dp, y * NZ + (z + d) % NZ)

    def at_y(d):
        return (dp, ((y + d) % NY) * NZ + z)

    def at_dp(d):
        return ((dp + d) % NDP, param)

    q_loads, t_loads = [], []
    for h in range(2):
        load = pltpu.make_async_copy(query.at[pl.ds(h * HALF, HALF), :], q.at[0, h], q_sem.at[h])
        load.start()
        q_loads.append(load)
    peers = [right, left, mate, at_z(1), at_z(NZ - 1), at_y(1), at_y(NY - 1)]
    barrier = pltpu.get_barrier_semaphore()
    for peer in peers:
        pl.semaphore_signal(barrier, inc=1, device_id=peer, device_id_type=pl.DeviceIdType.MESH)

    def squares(ref_rows, k):
        total = jnp.zeros((HALF, LANES), jnp.float32)
        for j in range(CUTS[k][1] // LANES):
            v = ref_rows(pl.ds(CUTS[k][0] + j * LANES, LANES)).astype(jnp.float32)
            total = total + v * v
        return total

    for load in q_loads:
        load.wait()
    for i in range(TRAIN // LANES):
        rows = pl.ds(i * LANES, LANES)
        load = pltpu.make_async_copy(train.at[rows, :], t.at[rows, :], t_sem.at[i])
        load.start()
        t_loads.append(load)
    own = []
    for h in range(2):
        total = squares(lambda s, h=h: q[0, h, :, s], 0)
        for k in range(1, NK):
            total = total + squares(lambda s, h=h: q[0, h, :, s], k)
        own.append(total)
    own += [jnp.zeros((LANES - 2 * HALF, LANES), jnp.float32)]
    qall[dp] = row_sums(jnp.concatenate(own, axis=0))

    pl.semaphore_wait(barrier, len(peers))

    def remote(src, dst, send, recv, to):
        return pltpu.make_async_remote_copy(
            src_ref=src, dst_ref=dst, send_sem=send, recv_sem=recv, device_id=to,
            device_id_type=pl.DeviceIdType.MESH,
        )

    def await_in(like, sem):
        remote(like, like, sem, sem, mate).wait_recv()

    def await_out(like, sem):
        remote(like, like, sem, sem, mate).wait_send()

    def hop(src, dst, h, k, recv, to):
        k0, w = CUTS[k]
        piece = pl.ds(k0, w)
        remote(q.at[src, h, :, piece], q.at[dst, h, :, piece], out_sem, recv, to).start()

    def tell(*steps):
        for i, whom in steps:
            for peer in whom:
                pl.semaphore_signal(far_sem.at[i], inc=1, device_id=peer, device_id_type=pl.DeviceIdType.MESH)

    def told(*steps):
        for i, whom in steps:
            pl.semaphore_wait(far_sem.at[i], len(whom))

    around = (right, left, mate)
    along_z, along_y = peers[3:5], peers[5:7]
    tell((0, around), (1, along_z), (2, along_y))
    for h in range(2):
        for k in range(NK):
            hop(0, 2, h, k, in_sem.at[h, k], right)
            hop(0, 4, h, k, in_sem.at[h, k], left)
        remote(q.at[0, h], q.at[1, h], out_sem, mate_sem, mate).start()

    def meet(step):
        if step == 0:
            told((0, around), (1, along_z), (2, along_y))
            tell((3, around), (4, along_z))
        elif step == 1:
            told((3, around), (4, along_z))
            tell((5, along_z))
        else:
            told((5, along_z))
            for d in range(1, NDP):
                remote(qall.at[dp], qall.at[dp], qn_send, qn_recv, at_dp(d)).start()

    def products(g, first, last):
        k0, w = CUTS[first][0], sum(WIDTHS[first:last])
        a = jnp.concatenate([q[s, h, :, pl.ds(k0, w)] for s, h in GROUPS[g]], axis=0)
        part = dot_rows(a, t[:, pl.ds(k0, w)])
        for i, (s, h) in enumerate(GROUPS[g]):
            piece = part[i * HALF : (i + 1) * HALF].reshape(2, 8, TRAIN)
            where = pl.ds(4 * s + 2 * h, 2)
            p[where] = piece if first == 0 else p[where] + piece

    def block_of(r, zt):
        return 4 * (2 * r + (zt // 4 + c) % 2) + zt % 4

    def z_copy(src, dst, sem, d):
        remote(src, dst, z_send, sem, at_z(d)).start()

    def mine(r, d):
        return p.at[block_of(r, (z + d) % NZ)]

    PLUS, MINUS = pl.ds(0, 512), pl.ds(512, TRAIN - 512)

    def send_z(*groups):
        for r in groups:
            z_copy(mine(r, 4).at[:, PLUS], zin.at[r, 6, :, PLUS], relay_recv.at[r], 2)
            z_copy(mine(r, 4).at[:, MINUS], zin.at[r, 6, :, MINUS], relay_recv.at[r], 6)
            z_copy(mine(r, 3), zin.at[r, 4], relay_recv.at[r], 1)
            z_copy(mine(r, 5), zin.at[r, 5], relay_recv.at[r], 7)
        for r in groups:
            z_copy(mine(r, 1), zin.at[r, 0], z_recv.at[r], 1)
            z_copy(mine(r, 7), zin.at[r, 1], z_recv.at[r], 7)

    def relay(r):
        await_in(zin.at[r, pl.ds(4, 3)], relay_recv.at[r])
        for i, (d, part) in enumerate(((2, PLUS), (6, MINUS))):
            zout[r, i] = p[block_of(r, (z + d) % NZ)] + zin[r, 4 + i]
            zout[r, i, :, part] += zin[r, 6, :, part]
            z_copy(zout.at[r, i], zin.at[r, 2 + i], z_recv.at[r], d)

    home = [x, (x + NX - 1) % NX, (x + 1) % NX, (x + 2) % NX]

    def send_y(r):
        await_in(zin.at[r, pl.ds(0, 4)], z_recv.at[r])
        total = p[block_of(r, z)]
        for i in range(4):
            total = total + zin[r, i]
        zsum[r] = total
        d = (home[r] + NY - y) % NY

        @pl.when(d != 0)
        def _():
            remote(zsum.at[r], yin.at[d - 1], y_send, y_recv, (dp, home[r] * NZ + z)).start()

    def arrive(g, k):
        k0, w = CUTS[k]
        await_in(q.at[2, :, :, pl.ds(k0, w)], in_sem.at[g, k])
        if g < 2:
            hop(2, 3, g, k, pass_sem.at[g, k], mate)
            hop(4, 5, g, k, pass_sem.at[g, k], mate)
            if g == 0:
                hop(2, 6, 0, k, in_sem.at[2, k], right)
            else:
                hop(4, 6, 1, k, in_sem.at[2, k], left)
        else:
            hop(6, 7, 0, k, pass_sem.at[2, k], mate)
            hop(6, 7, 1, k, pass_sem.at[2, k], mate)

    def multiply(g, first, last):
        if g == 0 and first == 0:
            await_in(q.at[1], mate_sem)
        for k in range(first, last):
            k0, w = CUTS[k]
            for part in ((), (0, 1), (2,))[g]:
                await_in(q.at[2, :, :, pl.ds(k0, w)], pass_sem.at[part, k])

        @pl.when(x >= 0)
        def _():
            products(g, first, last)

    def train_norms(first, last):
        def rows_of(i, carry):
            rows = pl.ds(pl.multiple_of(i * HALF, HALF), HALF)
            total = squares(lambda s: t[rows, s], 0)
            for k in range(1, NK):
                total = total + squares(lambda s, k=k: t[rows, s], k)
            tacc[rows, :] = total
            return carry

        for i in range(first, last):
            t_loads[i].wait()
            lax.fori_loop(i * LANES // HALF, (i + 1) * LANES // HALF, rows_of, 0)

    def send_norms():
        row = row_sums(tacc[...])
        await_in(qall.at[pl.ds(0, NDP - 1)], qn_recv)
        for i in range(NDP):
            norm[pl.ds(i, 1), :] = qall[i]
        for i in range(TRAIN // LANES):
            norm[pl.ds(NDP + i, 1), :] = row[:, i * LANES : (i + 1) * LANES]
        norm[pl.ds(15, 1), :] = jnp.zeros((1, LANES), jnp.float32)
        for d in FAR_FIRST:
            remote(norm, nz.at[d - 1], nz_send, nz_recv, at_z(d)).start()

    def add_norms():
        await_in(nz, nz_recv)
        total = norm[...]
        for d in range(NZ - 1):
            total = total + nz[d]
        nsum[...] = total
        for d in range(1, NY):
            remote(nsum, ny.at[d - 1], ny_send, ny_recv, at_y(d)).start()

    todo = [
        (train_norms, 0, 5),
        (meet, 0),
        (train_norms, 5, TRAIN // LANES),
        (meet, 1),
        (multiply, 0, 0, 2),
        (meet, 2),
        (arrive, 0, 0),
        (arrive, 0, 1),
        (multiply, 0, 2, 4),
        (send_z, 0),
        (arrive, 0, 2),
        (arrive, 0, 3),
        (arrive, 1, 0),
        (arrive, 1, 1),
        (multiply, 1, 0, 1),
        (arrive, 1, 2),
        (arrive, 1, 3),
        (multiply, 1, 1, 2),
        (relay, 0),
        (send_norms,),
        (arrive, 2, 0),
        (multiply, 1, 2, 4),
        (send_z, 1, 2),
        (arrive, 2, 1),
        (arrive, 2, 2),
        (multiply, 2, 0, 1),
        (add_norms,),
        (arrive, 2, 3),
        (multiply, 2, 1, 3),
        (multiply, 2, 3, 4),
        (send_z, 3),
        (send_y, 0),
        (relay, 1),
        (relay, 2),
        (relay, 3),
        (send_y, 1),
        (send_y, 2),
        (send_y, 3),
    ]
    for what, *how in todo:
        what(*how)

    await_in(ny, ny_recv)
    norms = nsum[...]
    for d in range(NY - 1):
        norms = norms + ny[d]
    nall[...] = norms
    train_norm = jnp.concatenate([norms[NDP + i : NDP + i + 1, :] for i in range(TRAIN // LANES)], axis=1)
    lane = lax.broadcasted_iota(jnp.int32, (8, LANES), 1)
    sub = lax.broadcasted_iota(jnp.int32, (8, LANES), 0)
    rows_norm = jnp.broadcast_to(nall[pl.ds(2 * y + z // 4, 1), :], (8, LANES))
    query_norm = jnp.sum(jnp.where(lane == sub + 8 * (z % 4), rows_norm, 0.0), axis=1, keepdims=True)
    query_scale = lax.rsqrt(query_norm + epsilon)
    train_scale = lax.rsqrt(train_norm + epsilon)

    ahead = (y + NX - x) % NX
    total = zsum[jnp.where(ahead == 0, 0, jnp.where(ahead == 3, 1, ahead + 1))]
    await_in(yin, y_recv)
    for d in range(NY - 1):
        total = total + yin[d]
    out[...] = total * query_scale * train_scale

    await_out(q.at[pl.ds(0, 7)], out_sem)
    await_out(zin, z_send)
    await_out(yin, y_send)
    await_out(qall.at[pl.ds(0, NDP - 1)], qn_send)
    await_out(nz, nz_send)
    await_out(ny, ny_send)


def per_device(train_grads, query_grads):
    f32, bf16 = jnp.float32, jnp.bfloat16
    dma = pltpu.SemaphoreType.DMA
    return pl.pallas_call(
        kernel,
        name="scores",
        out_shape=jax.ShapeDtypeStruct((8, TRAIN), f32),
        in_specs=[pl.BlockSpec(memory_space=pl.ANY)] * 2,
        out_specs=pl.BlockSpec(memory_space=pltpu.VMEM),
        scratch_shapes=[
            pltpu.VMEM((8, 2, HALF, DEPTH), bf16),
            pltpu.VMEM((TRAIN, DEPTH), bf16),
            pltpu.VMEM((32, 8, TRAIN), f32),
            pltpu.VMEM((4, NZ - 1, 8, TRAIN), f32),
            pltpu.VMEM((4, 2, 8, TRAIN), f32),
            pltpu.VMEM((4, 8, TRAIN), f32),
            pltpu.VMEM((NY - 1, 8, TRAIN), f32),
            pltpu.VMEM((TRAIN, LANES), f32),
            pltpu.VMEM((NDP, 1, LANES), f32),
            pltpu.VMEM((16, LANES), f32),
            pltpu.VMEM((NZ - 1, 16, LANES), f32),
            pltpu.VMEM((16, LANES), f32),
            pltpu.VMEM((NY - 1, 16, LANES), f32),
            pltpu.VMEM((16, LANES), f32),
            pltpu.SemaphoreType.REGULAR((6,)),
            dma((2,)),
            dma((TRAIN // LANES,)),
            dma(()),
            dma(()),
            dma((3, NK)),
            dma((3, NK)),
            dma(()),
            dma((4,)),
            dma((4,)),
        ]
        + [dma(())] * 8,
        compiler_params=pltpu.CompilerParams(
            collective_id=0, has_side_effects=True, vmem_limit_bytes=66_700_000
        ),
    )(train_grads, query_grads)


def solution(mesh):
    return jax.shard_map(
        per_device,
        mesh=mesh,
        in_specs=(P("dp", "param"), P("dp", "param")),
        out_specs=P("param", "dp"),
        check_vma=False,
    )
```

```python
import jax
import jax.numpy as jnp
from jax import lax
from jax.experimental import pallas as pl
from jax.experimental.pallas import tpu as pltpu
from jax.sharding import PartitionSpec as P

epsilon = 1e-06

NX, NY, NZ, NDP = 4, 4, 8, 8
TRAIN, DEPTH = 896, 6656
HALF = 16
LANES = 128
WIDTHS = (2048, 2048, 1536, 1024)
CUTS = tuple((sum(WIDTHS[:i]), w) for i, w in enumerate(WIDTHS))
NK = len(CUTS)
FAR_FIRST = (4, 3, 5, 2, 6, 1, 7)
GROUPS = (
    ((0, 0), (0, 1), (1, 0), (1, 1)),
    tuple((s, h) for s in range(2, 6) for h in range(2)),
    ((6, 0), (6, 1), (7, 0), (7, 1)),
)


def dot_rows(a, b):
    return lax.dot_general(a, b, (((1,), (1,)), ((), ())), preferred_element_type=jnp.float32)


def row_sums(lanes):
    high = lanes.astype(jnp.bfloat16)
    rest = lanes - high.astype(jnp.float32)
    mid = rest.astype(jnp.bfloat16)
    low = (rest - mid.astype(jnp.float32)).astype(jnp.bfloat16)
    ones = jnp.ones((16, 2 * LANES), jnp.bfloat16)
    both = jnp.concatenate([high, mid], axis=1)
    return (dot_rows(ones, both) + dot_rows(ones[:, :LANES], low))[0:1, :]


def kernel(
    train, query, out,
    q, t, p, zin, zout, zsum, yin, tacc, qall, norm, nz, nsum, ny, nall,
    far_sem, q_sem, t_sem, out_sem, mate_sem, in_sem, pass_sem,
    z_send, z_recv, relay_recv, y_send, y_recv, qn_send, qn_recv, nz_send, nz_recv, ny_send, ny_recv,
):
    dp, param = lax.axis_index("dp"), lax.axis_index("param")
    x, c = dp // 2, dp % 2
    y, z = param // NZ, param % NZ
    right = (((x + 1) % NX) * 2 + c, param)
    left = (((x + NX - 1) % NX) * 2 + c, param)
    mate = (x * 2 + 1 - c, param)

    def at_z(d):
        return (dp, y * NZ + (z + d) % NZ)

    def at_y(d):
        return (dp, ((y + d) % NY) * NZ + z)

    def at_dp(d):
        return ((dp + d) % NDP, param)

    q_loads, t_loads = [], []
    for h in range(2):
        load = pltpu.make_async_copy(query.at[pl.ds(h * HALF, HALF), :], q.at[0, h], q_sem.at[h])
        load.start()
        q_loads.append(load)
    peers = [right, left, mate, at_z(1), at_z(NZ - 1), at_y(1), at_y(NY - 1)]
    barrier = pltpu.get_barrier_semaphore()
    for peer in peers:
        pl.semaphore_signal(barrier, inc=1, device_id=peer, device_id_type=pl.DeviceIdType.MESH)

    def squares(ref_rows, k):
        total = jnp.zeros((HALF, LANES), jnp.float32)
        for j in range(CUTS[k][1] // LANES):
            v = ref_rows(pl.ds(CUTS[k][0] + j * LANES, LANES)).astype(jnp.float32)
            total = total + v * v
        return total

    for load in q_loads:
        load.wait()
    for i in range(TRAIN // LANES):
        rows = pl.ds(i * LANES, LANES)
        load = pltpu.make_async_copy(train.at[rows, :], t.at[rows, :], t_sem.at[i])
        load.start()
        t_loads.append(load)
    own = []
    for h in range(2):
        total = squares(lambda s, h=h: q[0, h, :, s], 0)
        for k in range(1, NK):
            total = total + squares(lambda s, h=h: q[0, h, :, s], k)
        own.append(total)
    own += [jnp.zeros((LANES - 2 * HALF, LANES), jnp.float32)]
    qall[dp] = row_sums(jnp.concatenate(own, axis=0))

    pl.semaphore_wait(barrier, len(peers))

    def remote(src, dst, send, recv, to):
        return pltpu.make_async_remote_copy(
            src_ref=src, dst_ref=dst, send_sem=send, recv_sem=recv, device_id=to,
            device_id_type=pl.DeviceIdType.MESH,
        )

    def await_in(like, sem):
        remote(like, like, sem, sem, mate).wait_recv()

    def await_out(like, sem):
        remote(like, like, sem, sem, mate).wait_send()

    def hop(src, dst, h, k, recv, to):
        k0, w = CUTS[k]
        piece = pl.ds(k0, w)
        remote(q.at[src, h, :, piece], q.at[dst, h, :, piece], out_sem, recv, to).start()

    def tell(*steps):
        for i, whom in steps:
            for peer in whom:
                pl.semaphore_signal(far_sem.at[i], inc=1, device_id=peer, device_id_type=pl.DeviceIdType.MESH)

    def told(*steps):
        for i, whom in steps:
            pl.semaphore_wait(far_sem.at[i], len(whom))

    around = (right, left, mate)
    along_z, along_y = peers[3:5], peers[5:7]
    tell((0, around), (1, along_z), (2, along_y))
    for h in range(2):
        for k in range(NK):
            hop(0, 2, h, k, in_sem.at[h, k], right)
            hop(0, 4, h, k, in_sem.at[h, k], left)
        remote(q.at[0, h], q.at[1, h], out_sem, mate_sem, mate).start()

    def meet(step):
        if step == 0:
            told((0, around), (1, along_z), (2, along_y))
            tell((3, around), (4, along_z))
        elif step == 1:
            told((3, around), (4, along_z))
            tell((5, along_z))
        else:
            told((5, along_z))
            for d in range(1, NDP):
                remote(qall.at[dp], qall.at[dp], qn_send, qn_recv, at_dp(d)).start()

    def products(g, first, last):
        k0, w = CUTS[first][0], sum(WIDTHS[first:last])
        a = jnp.concatenate([q[s, h, :, pl.ds(k0, w)] for s, h in GROUPS[g]], axis=0)
        part = dot_rows(a, t[:, pl.ds(k0, w)])
        for i, (s, h) in enumerate(GROUPS[g]):
            piece = part[i * HALF : (i + 1) * HALF].reshape(2, 8, TRAIN)
            where = pl.ds(4 * s + 2 * h, 2)
            p[where] = piece if first == 0 else p[where] + piece

    def block_of(r, zt):
        return 4 * (2 * r + (zt // 4 + c) % 2) + zt % 4

    def z_copy(src, dst, sem, d):
        remote(src, dst, z_send, sem, at_z(d)).start()

    def mine(r, d):
        return p.at[block_of(r, (z + d) % NZ)]

    PLUS, MINUS = pl.ds(0, 512), pl.ds(512, TRAIN - 512)

    def send_z(*groups):
        for r in groups:
            z_copy(mine(r, 4).at[:, PLUS], zin.at[r, 6, :, PLUS], relay_recv.at[r], 2)
            z_copy(mine(r, 4).at[:, MINUS], zin.at[r, 6, :, MINUS], relay_recv.at[r], 6)
            z_copy(mine(r, 3), zin.at[r, 4], relay_recv.at[r], 1)
            z_copy(mine(r, 5), zin.at[r, 5], relay_recv.at[r], 7)
        for r in groups:
            z_copy(mine(r, 1), zin.at[r, 0], z_recv.at[r], 1)
            z_copy(mine(r, 7), zin.at[r, 1], z_recv.at[r], 7)

    def relay(r):
        await_in(zin.at[r, pl.ds(4, 3)], relay_recv.at[r])
        for i, (d, part) in enumerate(((2, PLUS), (6, MINUS))):
            zout[r, i] = p[block_of(r, (z + d) % NZ)] + zin[r, 4 + i]
            zout[r, i, :, part] += zin[r, 6, :, part]
            z_copy(zout.at[r, i], zin.at[r, 2 + i], z_recv.at[r], d)

    home = [x, (x + NX - 1) % NX, (x + 1) % NX, (x + 2) % NX]

    def send_y(r):
        await_in(zin.at[r, pl.ds(0, 4)], z_recv.at[r])
        total = p[block_of(r, z)]
        for i in range(4):
            total = total + zin[r, i]
        zsum[r] = total
        d = (home[r] + NY - y) % NY

        @pl.when(d != 0)
        def _():
            remote(zsum.at[r], yin.at[d - 1], y_send, y_recv, (dp, home[r] * NZ + z)).start()

    def arrive(g, k):
        k0, w = CUTS[k]
        await_in(q.at[2, :, :, pl.ds(k0, w)], in_sem.at[g, k])
        if g < 2:
            hop(2, 3, g, k, pass_sem.at[g, k], mate)
            hop(4, 5, g, k, pass_sem.at[g, k], mate)
            if g == 0:
                hop(2, 6, 0, k, in_sem.at[2, k], right)
            else:
                hop(4, 6, 1, k, in_sem.at[2, k], left)
        else:
            hop(6, 7, 0, k, pass_sem.at[2, k], mate)
            hop(6, 7, 1, k, pass_sem.at[2, k], mate)

    def multiply(g, first, last):
        if g == 0 and first == 0:
            await_in(q.at[1], mate_sem)
        for k in range(first, last):
            k0, w = CUTS[k]
            for part in ((), (0, 1), (2,))[g]:
                await_in(q.at[2, :, :, pl.ds(k0, w)], pass_sem.at[part, k])

        @pl.when(x >= 0)
        def _():
            products(g, first, last)

    def train_norms(first, last):
        def rows_of(i, carry):
            rows = pl.ds(pl.multiple_of(i * HALF, HALF), HALF)
            total = squares(lambda s: t[rows, s], 0)
            for k in range(1, NK):
                total = total + squares(lambda s, k=k: t[rows, s], k)
            tacc[rows, :] = total
            return carry

        for i in range(first, last):
            t_loads[i].wait()
            lax.fori_loop(i * LANES // HALF, (i + 1) * LANES // HALF, rows_of, 0)

    def fill_norms():
        row = row_sums(tacc[...])
        for i in range(TRAIN // LANES):
            norm[pl.ds(NDP + i, 1), :] = row[:, i * LANES : (i + 1) * LANES]
        norm[pl.ds(15, 1), :] = jnp.zeros((1, LANES), jnp.float32)

    def send_norms():
        await_in(qall.at[pl.ds(0, NDP - 1)], qn_recv)
        for i in range(NDP):
            norm[pl.ds(i, 1), :] = qall[i]
        for d in FAR_FIRST:
            remote(norm, nz.at[d - 1], nz_send, nz_recv, at_z(d)).start()

    def add_norms():
        await_in(nz, nz_recv)
        total = norm[...]
        for d in range(NZ - 1):
            total = total + nz[d]
        nsum[...] = total
        for d in range(1, NY):
            remote(nsum, ny.at[d - 1], ny_send, ny_recv, at_y(d)).start()

    todo = [
        (train_norms, 0, 5),
        (meet, 0),
        (train_norms, 5, TRAIN // LANES),
        (fill_norms,),
        (meet, 1),
        (multiply, 0, 0, 2),
        (meet, 2),
        (arrive, 0, 0),
        (arrive, 0, 1),
        (multiply, 0, 2, 4),
        (send_z, 0),
        (arrive, 0, 2),
        (arrive, 0, 3),
        (arrive, 1, 0),
        (arrive, 1, 1),
        (multiply, 1, 0, 1),
        (arrive, 1, 2),
        (arrive, 1, 3),
        (multiply, 1, 1, 2),
        (relay, 0),
        (send_norms,),
        (arrive, 2, 0),
        (multiply, 1, 2, 4),
        (send_z, 1, 2),
        (arrive, 2, 1),
        (arrive, 2, 2),
        (multiply, 2, 0, 1),
        (arrive, 2, 3),
        (multiply, 2, 1, 3),
        (multiply, 2, 3, 4),
        (send_z, 3),
        (send_y, 0),
        (relay, 1),
        (relay, 2),
        (relay, 3),
        (add_norms,),
        (send_y, 1),
        (send_y, 2),
        (send_y, 3),
    ]
    for what, *how in todo:
        what(*how)

    await_in(ny, ny_recv)
    norms = nsum[...]
    for d in range(NY - 1):
        norms = norms + ny[d]
    nall[...] = norms
    train_norm = jnp.concatenate([norms[NDP + i : NDP + i + 1, :] for i in range(TRAIN // LANES)], axis=1)
    lane = lax.broadcasted_iota(jnp.int32, (8, LANES), 1)
    sub = lax.broadcasted_iota(jnp.int32, (8, LANES), 0)
    rows_norm = jnp.broadcast_to(nall[pl.ds(2 * y + z // 4, 1), :], (8, LANES))
    query_norm = jnp.sum(jnp.where(lane == sub + 8 * (z % 4), rows_norm, 0.0), axis=1, keepdims=True)
    query_scale = lax.rsqrt(query_norm + epsilon)
    train_scale = lax.rsqrt(train_norm + epsilon)

    ahead = (y + NX - x) % NX
    total = zsum[jnp.where(ahead == 0, 0, jnp.where(ahead == 3, 1, ahead + 1))]
    await_in(yin, y_recv)
    for d in range(NY - 1):
        total = total + yin[d]
    out[...] = total * query_scale * train_scale

    await_out(q.at[pl.ds(0, 7)], out_sem)
    await_out(zin, z_send)
    await_out(yin, y_send)
    await_out(qall.at[pl.ds(0, NDP - 1)], qn_send)
    await_out(nz, nz_send)
    await_out(ny, ny_send)


def per_device(train_grads, query_grads):
    f32, bf16 = jnp.float32, jnp.bfloat16
    dma = pltpu.SemaphoreType.DMA
    return pl.pallas_call(
        kernel,
        name="scores",
        out_shape=jax.ShapeDtypeStruct((8, TRAIN), f32),
        in_specs=[pl.BlockSpec(memory_space=pl.ANY)] * 2,
        out_specs=pl.BlockSpec(memory_space=pltpu.VMEM),
        scratch_shapes=[
            pltpu.VMEM((8, 2, HALF, DEPTH), bf16),
            pltpu.VMEM((TRAIN, DEPTH), bf16),
            pltpu.VMEM((32, 8, TRAIN), f32),
            pltpu.VMEM((4, NZ - 1, 8, TRAIN), f32),
            pltpu.VMEM((4, 2, 8, TRAIN), f32),
            pltpu.VMEM((4, 8, TRAIN), f32),
            pltpu.VMEM((NY - 1, 8, TRAIN), f32),
            pltpu.VMEM((TRAIN, LANES), f32),
            pltpu.VMEM((NDP, 1, LANES), f32),
            pltpu.VMEM((16, LANES), f32),
            pltpu.VMEM((NZ - 1, 16, LANES), f32),
            pltpu.VMEM((16, LANES), f32),
            pltpu.VMEM((NY - 1, 16, LANES), f32),
            pltpu.VMEM((16, LANES), f32),
            pltpu.SemaphoreType.REGULAR((6,)),
            dma((2,)),
            dma((TRAIN // LANES,)),
            dma(()),
            dma(()),
            dma((3, NK)),
            dma((3, NK)),
            dma(()),
            dma((4,)),
            dma((4,)),
        ]
        + [dma(())] * 8,
        compiler_params=pltpu.CompilerParams(
            collective_id=0, has_side_effects=True, vmem_limit_bytes=66_700_000
        ),
    )(train_grads, query_grads)


def solution(mesh):
    return jax.shard_map(
        per_device,
        mesh=mesh,
        in_specs=(P("dp", "param"), P("dp", "param")),
        out_specs=P("param", "dp"),
        check_vma=False,
    )
```

```python
import jax
import jax.numpy as jnp
from jax import lax
from jax.experimental import pallas as pl
from jax.experimental.pallas import tpu as pltpu
from jax.sharding import PartitionSpec as P

epsilon = 1e-06

NX, NY, NZ, NDP = 4, 4, 8, 8
TRAIN, DEPTH = 896, 6656
HALF = 16
LANES = 128
WIDTHS = (2048, 2048, 1536, 1024)
CUTS = tuple((sum(WIDTHS[:i]), w) for i, w in enumerate(WIDTHS))
NK = len(CUTS)
FAR_FIRST = (4, 3, 5, 2, 6, 1, 7)
GROUPS = (
    ((0, 0), (0, 1), (1, 0), (1, 1)),
    tuple((s, h) for s in range(2, 6) for h in range(2)),
    ((6, 0), (6, 1), (7, 0), (7, 1)),
)


def dot_rows(a, b):
    return lax.dot_general(a, b, (((1,), (1,)), ((), ())), preferred_element_type=jnp.float32)


def row_sums(lanes):
    high = lanes.astype(jnp.bfloat16)
    rest = lanes - high.astype(jnp.float32)
    mid = rest.astype(jnp.bfloat16)
    low = (rest - mid.astype(jnp.float32)).astype(jnp.bfloat16)
    ones = jnp.ones((16, 2 * LANES), jnp.bfloat16)
    both = jnp.concatenate([high, mid], axis=1)
    return (dot_rows(ones, both) + dot_rows(ones[:, :LANES], low))[0:1, :]


def kernel(
    train, query, out,
    q, t, p, zin, zout, zsum, yin, tacc, qall, norm, nz, nsum, ny, nall,
    far_sem, q_sem, t_sem, out_sem, mate_sem, in_sem, pass_sem,
    z_send, z_recv, relay_recv, y_send, y_recv, qn_send, qn_recv, nz_send, nz_recv, ny_send, ny_recv,
):
    dp, param = lax.axis_index("dp"), lax.axis_index("param")
    x, c = dp // 2, dp % 2
    y, z = param // NZ, param % NZ
    right = (((x + 1) % NX) * 2 + c, param)
    left = (((x + NX - 1) % NX) * 2 + c, param)
    mate = (x * 2 + 1 - c, param)

    def at_z(d):
        return (dp, y * NZ + (z + d) % NZ)

    def at_y(d):
        return (dp, ((y + d) % NY) * NZ + z)

    def at_dp(d):
        return ((dp + d) % NDP, param)

    q_loads, t_loads = [], []
    for h in range(2):
        load = pltpu.make_async_copy(query.at[pl.ds(h * HALF, HALF), :], q.at[0, h], q_sem.at[h])
        load.start()
        q_loads.append(load)
    peers = [right, left, mate, at_z(1), at_z(NZ - 1), at_y(1), at_y(NY - 1)]
    barrier = pltpu.get_barrier_semaphore()
    for peer in peers:
        pl.semaphore_signal(barrier, inc=1, device_id=peer, device_id_type=pl.DeviceIdType.MESH)

    def squares(ref_rows, k):
        total = jnp.zeros((HALF, LANES), jnp.float32)
        for j in range(CUTS[k][1] // LANES):
            v = ref_rows(pl.ds(CUTS[k][0] + j * LANES, LANES)).astype(jnp.float32)
            total = total + v * v
        return total

    for load in q_loads:
        load.wait()
    for i in range(TRAIN // LANES):
        rows = pl.ds(i * LANES, LANES)
        load = pltpu.make_async_copy(train.at[rows, :], t.at[rows, :], t_sem.at[i])
        load.start()
        t_loads.append(load)
    own = []
    for h in range(2):
        total = squares(lambda s, h=h: q[0, h, :, s], 0)
        for k in range(1, NK):
            total = total + squares(lambda s, h=h: q[0, h, :, s], k)
        own.append(total)
    own += [jnp.zeros((LANES - 2 * HALF, LANES), jnp.float32)]
    qall[dp] = row_sums(jnp.concatenate(own, axis=0))

    pl.semaphore_wait(barrier, len(peers))

    def remote(src, dst, send, recv, to):
        return pltpu.make_async_remote_copy(
            src_ref=src, dst_ref=dst, send_sem=send, recv_sem=recv, device_id=to,
            device_id_type=pl.DeviceIdType.MESH,
        )

    def await_in(like, sem):
        remote(like, like, sem, sem, mate).wait_recv()

    def await_out(like, sem):
        remote(like, like, sem, sem, mate).wait_send()

    def hop(src, dst, h, k, recv, to):
        k0, w = CUTS[k]
        piece = pl.ds(k0, w)
        remote(q.at[src, h, :, piece], q.at[dst, h, :, piece], out_sem, recv, to).start()

    def tell(*steps):
        for i, whom in steps:
            for peer in whom:
                pl.semaphore_signal(far_sem.at[i], inc=1, device_id=peer, device_id_type=pl.DeviceIdType.MESH)

    def told(*steps):
        for i, whom in steps:
            pl.semaphore_wait(far_sem.at[i], len(whom))

    around = (right, left, mate)
    along_z, along_y = peers[3:5], peers[5:7]
    tell((0, around), (1, along_z), (2, along_y))
    for k in range(NK):
        for h in range(2):
            hop(0, 2, h, k, in_sem.at[0, k], right)
            hop(0, 4, h, k, in_sem.at[0, k], left)
    for h in range(2):
        remote(q.at[0, h], q.at[1, h], out_sem, mate_sem, mate).start()

    def meet(step):
        if step == 0:
            told((0, around), (1, along_z), (2, along_y))
            tell((3, around), (4, along_z))
        elif step == 1:
            told((3, around), (4, along_z))
            tell((5, along_z))
        else:
            told((5, along_z))
            for d in range(1, NDP):
                remote(qall.at[dp], qall.at[dp], qn_send, qn_recv, at_dp(d)).start()

    def products(g, first, last):
        k0, w = CUTS[first][0], sum(WIDTHS[first:last])
        a = jnp.concatenate([q[s, h, :, pl.ds(k0, w)] for s, h in GROUPS[g]], axis=0)
        part = dot_rows(a, t[:, pl.ds(k0, w)])
        for i, (s, h) in enumerate(GROUPS[g]):
            piece = part[i * HALF : (i + 1) * HALF].reshape(2, 8, TRAIN)
            where = pl.ds(4 * s + 2 * h, 2)
            p[where] = piece if first == 0 else p[where] + piece

    def block_of(r, zt):
        return 4 * (2 * r + (zt // 4 + c) % 2) + zt % 4

    def z_copy(src, dst, sem, d):
        remote(src, dst, z_send, sem, at_z(d)).start()

    def mine(r, d):
        return p.at[block_of(r, (z + d) % NZ)]

    PLUS, MINUS = pl.ds(0, 512), pl.ds(512, TRAIN - 512)

    def send_z(*groups):
        for r in groups:
            z_copy(mine(r, 4).at[:, PLUS], zin.at[r, 6, :, PLUS], relay_recv.at[r], 2)
            z_copy(mine(r, 4).at[:, MINUS], zin.at[r, 6, :, MINUS], relay_recv.at[r], 6)
            z_copy(mine(r, 3), zin.at[r, 4], relay_recv.at[r], 1)
            z_copy(mine(r, 5), zin.at[r, 5], relay_recv.at[r], 7)
        for r in groups:
            z_copy(mine(r, 1), zin.at[r, 0], z_recv.at[r], 1)
            z_copy(mine(r, 7), zin.at[r, 1], z_recv.at[r], 7)

    def relay(r):
        await_in(zin.at[r, pl.ds(4, 3)], relay_recv.at[r])
        for i, (d, part) in enumerate(((2, PLUS), (6, MINUS))):
            zout[r, i] = p[block_of(r, (z + d) % NZ)] + zin[r, 4 + i]
            zout[r, i, :, part] += zin[r, 6, :, part]
            z_copy(zout.at[r, i], zin.at[r, 2 + i], z_recv.at[r], d)

    home = [x, (x + NX - 1) % NX, (x + 1) % NX, (x + 2) % NX]

    def send_y(r):
        await_in(zin.at[r, pl.ds(0, 4)], z_recv.at[r])
        total = p[block_of(r, z)]
        for i in range(4):
            total = total + zin[r, i]
        zsum[r] = total
        d = (home[r] + NY - y) % NY

        @pl.when(d != 0)
        def _():
            remote(zsum.at[r], yin.at[d - 1], y_send, y_recv, (dp, home[r] * NZ + z)).start()

    def pieces(g, k):
        return q.at[pl.ds(2, 2) if g == 1 else 2, :, :, pl.ds(*CUTS[k])]

    def arrive(g, k):
        await_in(pieces(g, k), in_sem.at[g - 1, k])
        for h in range(2):
            if g == 1:
                hop(2, 3, h, k, pass_sem.at[0, k], mate)
                hop(4, 5, h, k, pass_sem.at[0, k], mate)
            else:
                hop(6, 7, h, k, pass_sem.at[1, k], mate)
        if g == 1:
            hop(2, 6, 0, k, in_sem.at[1, k], right)
            hop(4, 6, 1, k, in_sem.at[1, k], left)

    def multiply(g, first, last):
        if g == 0 and first == 0:
            await_in(q.at[1], mate_sem)
        if g > 0:
            for k in range(first, last):
                await_in(pieces(g, k), pass_sem.at[g - 1, k])

        @pl.when(x >= 0)
        def _():
            products(g, first, last)

    def train_norms(first, last):
        def rows_of(i, carry):
            rows = pl.ds(pl.multiple_of(i * HALF, HALF), HALF)
            total = squares(lambda s: t[rows, s], 0)
            for k in range(1, NK):
                total = total + squares(lambda s, k=k: t[rows, s], k)
            tacc[rows, :] = total
            return carry

        for i in range(first, last):
            t_loads[i].wait()
            lax.fori_loop(i * LANES // HALF, (i + 1) * LANES // HALF, rows_of, 0)

    def fill_norms():
        row = row_sums(tacc[...])
        for i in range(TRAIN // LANES):
            norm[pl.ds(NDP + i, 1), :] = row[:, i * LANES : (i + 1) * LANES]
        norm[pl.ds(15, 1), :] = jnp.zeros((1, LANES), jnp.float32)

    def send_norms():
        await_in(qall.at[pl.ds(0, NDP - 1)], qn_recv)
        for i in range(NDP):
            norm[pl.ds(i, 1), :] = qall[i]
        for d in FAR_FIRST:
            remote(norm, nz.at[d - 1], nz_send, nz_recv, at_z(d)).start()

    def add_norms():
        await_in(nz, nz_recv)
        total = norm[...]
        for d in range(NZ - 1):
            total = total + nz[d]
        nsum[...] = total
        for d in range(1, NY):
            remote(nsum, ny.at[d - 1], ny_send, ny_recv, at_y(d)).start()

    todo = [
        (train_norms, 0, 5),
        (meet, 0),
        (train_norms, 5, TRAIN // LANES),
        (fill_norms,),
        (meet, 1),
        (multiply, 0, 0, 2),
        (meet, 2),
        (arrive, 1, 0),
        (multiply, 0, 2, 4),
        (send_z, 0),
        (arrive, 1, 1),
        (multiply, 1, 0, 1),
        (arrive, 1, 2),
        (multiply, 1, 1, 2),
        (relay, 0),
        (send_norms,),
        (arrive, 1, 3),
        (multiply, 1, 2, 3),
        (arrive, 2, 0),
        (multiply, 1, 3, 4),
        (send_z, 1, 2),
        (arrive, 2, 1),
        (multiply, 2, 0, 1),
        (arrive, 2, 2),
        (multiply, 2, 1, 2),
        (arrive, 2, 3),
        (multiply, 2, 2, 3),
        (multiply, 2, 3, 4),
        (send_z, 3),
        (send_y, 0),
        (relay, 1),
        (relay, 2),
        (relay, 3),
        (add_norms,),
        (send_y, 1),
        (send_y, 2),
        (send_y, 3),
    ]
    for what, *how in todo:
        what(*how)

    await_in(ny, ny_recv)
    norms = nsum[...]
    for d in range(NY - 1):
        norms = norms + ny[d]
    nall[...] = norms
    train_norm = jnp.concatenate([norms[NDP + i : NDP + i + 1, :] for i in range(TRAIN // LANES)], axis=1)
    lane = lax.broadcasted_iota(jnp.int32, (8, LANES), 1)
    sub = lax.broadcasted_iota(jnp.int32, (8, LANES), 0)
    rows_norm = jnp.broadcast_to(nall[pl.ds(2 * y + z // 4, 1), :], (8, LANES))
    query_norm = jnp.sum(jnp.where(lane == sub + 8 * (z % 4), rows_norm, 0.0), axis=1, keepdims=True)
    query_scale = lax.rsqrt(query_norm + epsilon)
    train_scale = lax.rsqrt(train_norm + epsilon)

    ahead = (y + NX - x) % NX
    total = zsum[jnp.where(ahead == 0, 0, jnp.where(ahead == 3, 1, ahead + 1))]
    await_in(yin, y_recv)
    for d in range(NY - 1):
        total = total + yin[d]
    out[...] = total * query_scale * train_scale

    await_out(q.at[pl.ds(0, 7)], out_sem)
    await_out(zin, z_send)
    await_out(yin, y_send)
    await_out(qall.at[pl.ds(0, NDP - 1)], qn_send)
    await_out(nz, nz_send)
    await_out(ny, ny_send)


def per_device(train_grads, query_grads):
    f32, bf16 = jnp.float32, jnp.bfloat16
    dma = pltpu.SemaphoreType.DMA
    return pl.pallas_call(
        kernel,
        name="scores",
        out_shape=jax.ShapeDtypeStruct((8, TRAIN), f32),
        in_specs=[pl.BlockSpec(memory_space=pl.ANY)] * 2,
        out_specs=pl.BlockSpec(memory_space=pltpu.VMEM),
        scratch_shapes=[
            pltpu.VMEM((8, 2, HALF, DEPTH), bf16),
            pltpu.VMEM((TRAIN, DEPTH), bf16),
            pltpu.VMEM((32, 8, TRAIN), f32),
            pltpu.VMEM((4, NZ - 1, 8, TRAIN), f32),
            pltpu.VMEM((4, 2, 8, TRAIN), f32),
            pltpu.VMEM((4, 8, TRAIN), f32),
            pltpu.VMEM((NY - 1, 8, TRAIN), f32),
            pltpu.VMEM((TRAIN, LANES), f32),
            pltpu.VMEM((NDP, 1, LANES), f32),
            pltpu.VMEM((16, LANES), f32),
            pltpu.VMEM((NZ - 1, 16, LANES), f32),
            pltpu.VMEM((16, LANES), f32),
            pltpu.VMEM((NY - 1, 16, LANES), f32),
            pltpu.VMEM((16, LANES), f32),
            pltpu.SemaphoreType.REGULAR((6,)),
            dma((2,)),
            dma((TRAIN // LANES,)),
            dma(()),
            dma(()),
            dma((2, NK)),
            dma((2, NK)),
            dma(()),
            dma((4,)),
            dma((4,)),
        ]
        + [dma(())] * 8,
        compiler_params=pltpu.CompilerParams(
            collective_id=0, has_side_effects=True, vmem_limit_bytes=66_700_000
        ),
    )(train_grads, query_grads)


def solution(mesh):
    return jax.shard_map(
        per_device,
        mesh=mesh,
        in_specs=(P("dp", "param"), P("dp", "param")),
        out_specs=P("param", "dp"),
        check_vma=False,
    )
```

```python
import jax
import jax.numpy as jnp
from jax import lax
from jax.experimental import pallas as pl
from jax.experimental.pallas import tpu as pltpu
from jax.sharding import PartitionSpec as P

epsilon = 1e-06

NX, NY, NZ, NDP = 4, 4, 8, 8
TRAIN, DEPTH = 896, 6656
HALF = 16
LANES = 128
WIDTHS = (2048, 2048, 1536, 1024)
CUTS = tuple((sum(WIDTHS[:i]), w) for i, w in enumerate(WIDTHS))
NK = len(CUTS)
FAR_FIRST = (4, 3, 5, 2, 6, 1, 7)
GROUPS = (
    ((0, 0), (0, 1), (1, 0), (1, 1)),
    tuple((s, h) for s in range(2, 6) for h in range(2)),
    ((6, 0), (6, 1), (7, 0), (7, 1)),
)


def dot_rows(a, b):
    return lax.dot_general(a, b, (((1,), (1,)), ((), ())), preferred_element_type=jnp.float32)


def row_sums(lanes):
    high = lanes.astype(jnp.bfloat16)
    rest = lanes - high.astype(jnp.float32)
    mid = rest.astype(jnp.bfloat16)
    low = (rest - mid.astype(jnp.float32)).astype(jnp.bfloat16)
    ones = jnp.ones((16, 2 * LANES), jnp.bfloat16)
    both = jnp.concatenate([high, mid], axis=1)
    return (dot_rows(ones, both) + dot_rows(ones[:, :LANES], low))[0:1, :]


def kernel(
    train, query, out,
    q, t, p, zin, zout, zsum, yin, tacc, qall, norm, nz, nsum, ny, nall,
    far_sem, q_sem, t_sem, out_sem, mate_sem, in_sem, pass_sem,
    z_send, z_recv, relay_recv, y_send, y_recv, qn_send, qn_recv, nz_send, nz_recv, ny_send, ny_recv,
):
    dp, param = lax.axis_index("dp"), lax.axis_index("param")
    x, c = dp // 2, dp % 2
    y, z = param // NZ, param % NZ
    right = (((x + 1) % NX) * 2 + c, param)
    left = (((x + NX - 1) % NX) * 2 + c, param)
    mate = (x * 2 + 1 - c, param)

    def at_z(d):
        return (dp, y * NZ + (z + d) % NZ)

    def at_y(d):
        return (dp, ((y + d) % NY) * NZ + z)

    def at_dp(d):
        return ((dp + d) % NDP, param)

    q_loads, t_loads = [], []
    for h in range(2):
        load = pltpu.make_async_copy(query.at[pl.ds(h * HALF, HALF), :], q.at[0, h], q_sem.at[h])
        load.start()
        q_loads.append(load)
    peers = [right, left, mate, at_z(1), at_z(NZ - 1), at_y(1), at_y(NY - 1)]
    barrier = pltpu.get_barrier_semaphore()
    for peer in peers:
        pl.semaphore_signal(barrier, inc=1, device_id=peer, device_id_type=pl.DeviceIdType.MESH)

    def squares(ref_rows, k):
        total = jnp.zeros((HALF, LANES), jnp.float32)
        for j in range(CUTS[k][1] // LANES):
            v = ref_rows(pl.ds(CUTS[k][0] + j * LANES, LANES)).astype(jnp.float32)
            total = total + v * v
        return total

    for load in q_loads:
        load.wait()
    for i in range(TRAIN // LANES):
        rows = pl.ds(i * LANES, LANES)
        load = pltpu.make_async_copy(train.at[rows, :], t.at[rows, :], t_sem.at[i])
        load.start()
        t_loads.append(load)
    own = []
    for h in range(2):
        total = squares(lambda s, h=h: q[0, h, :, s], 0)
        for k in range(1, NK):
            total = total + squares(lambda s, h=h: q[0, h, :, s], k)
        own.append(total)
    own += [jnp.zeros((LANES - 2 * HALF, LANES), jnp.float32)]
    qall[dp] = row_sums(jnp.concatenate(own, axis=0))

    pl.semaphore_wait(barrier, len(peers))

    def remote(src, dst, send, recv, to):
        return pltpu.make_async_remote_copy(
            src_ref=src, dst_ref=dst, send_sem=send, recv_sem=recv, device_id=to,
            device_id_type=pl.DeviceIdType.MESH,
        )

    def await_in(like, sem):
        remote(like, like, sem, sem, mate).wait_recv()

    def await_out(like, sem):
        remote(like, like, sem, sem, mate).wait_send()

    def hop(src, dst, h, k, recv, to):
        k0, w = CUTS[k]
        piece = pl.ds(k0, w)
        remote(q.at[src, h, :, piece], q.at[dst, h, :, piece], out_sem, recv, to).start()

    def tell(*steps):
        for i, whom in steps:
            for peer in whom:
                pl.semaphore_signal(far_sem.at[i], inc=1, device_id=peer, device_id_type=pl.DeviceIdType.MESH)

    def told(*steps):
        for i, whom in steps:
            pl.semaphore_wait(far_sem.at[i], len(whom))

    around = (right, left, mate)
    along_z, along_y = peers[3:5], peers[5:7]
    tell((0, around), (1, along_z), (2, along_y))
    for k in range(NK):
        for h in range(2):
            hop(0, 2, h, k, in_sem.at[0, k], right)
            hop(0, 4, h, k, in_sem.at[0, k], left)
    for h in range(2):
        remote(q.at[0, h], q.at[1, h], out_sem, mate_sem, mate).start()

    def meet(step):
        if step == 0:
            told((0, around), (1, along_z), (2, along_y))
            tell((3, around), (4, along_z))
        elif step == 1:
            told((3, around), (4, along_z))
            tell((5, along_z))
        else:
            told((5, along_z))
            for d in range(1, NDP):
                remote(qall.at[dp], qall.at[dp], qn_send, qn_recv, at_dp(d)).start()

    def products(g, first, last):
        k0, w = CUTS[first][0], sum(WIDTHS[first:last])
        a = jnp.concatenate([q[s, h, :, pl.ds(k0, w)] for s, h in GROUPS[g]], axis=0)
        part = dot_rows(a, t[:, pl.ds(k0, w)])
        for i, (s, h) in enumerate(GROUPS[g]):
            piece = part[i * HALF : (i + 1) * HALF].reshape(2, 8, TRAIN)
            where = pl.ds(4 * s + 2 * h, 2)
            p[where] = piece if first == 0 else p[where] + piece

    def block_of(r, zt):
        return 4 * (2 * r + (zt // 4 + c) % 2) + zt % 4

    def z_copy(src, dst, sem, d):
        remote(src, dst, z_send, sem, at_z(d)).start()

    def mine(r, d):
        return p.at[block_of(r, (z + d) % NZ)]

    PLUS, MINUS = pl.ds(0, 512), pl.ds(512, TRAIN - 512)

    def send_z(*groups):
        for r in groups:
            z_copy(mine(r, 4).at[:, PLUS], zin.at[r, 6, :, PLUS], relay_recv.at[r], 2)
            z_copy(mine(r, 4).at[:, MINUS], zin.at[r, 6, :, MINUS], relay_recv.at[r], 6)
            z_copy(mine(r, 3), zin.at[r, 4], relay_recv.at[r], 1)
            z_copy(mine(r, 5), zin.at[r, 5], relay_recv.at[r], 7)
        for r in groups:
            z_copy(mine(r, 1), zin.at[r, 0], z_recv.at[r], 1)
            z_copy(mine(r, 7), zin.at[r, 1], z_recv.at[r], 7)

    def relay(r):
        await_in(zin.at[r, pl.ds(4, 3)], relay_recv.at[r])
        for i, (d, part) in enumerate(((2, PLUS), (6, MINUS))):
            zout[r, i] = p[block_of(r, (z + d) % NZ)] + zin[r, 4 + i]
            zout[r, i, :, part] += zin[r, 6, :, part]
            z_copy(zout.at[r, i], zin.at[r, 2 + i], z_recv.at[r], d)

    home = [x, (x + NX - 1) % NX, (x + 1) % NX, (x + 2) % NX]

    def send_y(r):
        await_in(zin.at[r, pl.ds(0, 4)], z_recv.at[r])
        total = p[block_of(r, z)]
        for i in range(4):
            total = total + zin[r, i]
        zsum[r] = total
        d = (home[r] + NY - y) % NY

        @pl.when(d != 0)
        def _():
            remote(zsum.at[r], yin.at[d - 1], y_send, y_recv, (dp, home[r] * NZ + z)).start()

    def pieces(g, k):
        return q.at[pl.ds(2, 2) if g == 1 else 2, :, :, pl.ds(*CUTS[k])]

    def arrive(g, k):
        await_in(pieces(g, k), in_sem.at[g - 1, k])
        for h in range(2):
            if g == 1:
                hop(2, 3, h, k, pass_sem.at[0, k], mate)
                hop(4, 5, h, k, pass_sem.at[0, k], mate)
            else:
                hop(6, 7, h, k, pass_sem.at[1, k], mate)
        if g == 1:
            hop(2, 6, 0, k, in_sem.at[1, k], right)
            hop(4, 6, 1, k, in_sem.at[1, k], left)

    def multiply(g, first, last):
        if g == 0 and first == 0:
            await_in(q.at[1], mate_sem)
        if g > 0:
            for k in range(first, last):
                await_in(pieces(g, k), pass_sem.at[g - 1, k])

        @pl.when(x >= 0)
        def _():
            products(g, first, last)

    def train_norms(first, last):
        def rows_of(i, carry):
            rows = pl.ds(pl.multiple_of(i * HALF, HALF), HALF)
            total = squares(lambda s: t[rows, s], 0)
            for k in range(1, NK):
                total = total + squares(lambda s, k=k: t[rows, s], k)
            tacc[rows, :] = total
            return carry

        for i in range(first, last):
            t_loads[i].wait()
            lax.fori_loop(i * LANES // HALF, (i + 1) * LANES // HALF, rows_of, 0)

    def fill_norms():
        row = row_sums(tacc[...])
        for i in range(TRAIN // LANES):
            norm[pl.ds(NDP + i, 1), :] = row[:, i * LANES : (i + 1) * LANES]
        norm[pl.ds(15, 1), :] = jnp.zeros((1, LANES), jnp.float32)

    def send_norms():
        await_in(qall.at[pl.ds(0, NDP - 1)], qn_recv)
        for i in range(NDP):
            norm[pl.ds(i, 1), :] = qall[i]
        for d in FAR_FIRST:
            remote(norm, nz.at[d - 1], nz_send, nz_recv, at_z(d)).start()

    def add_norms():
        await_in(nz, nz_recv)
        total = norm[...]
        for d in range(NZ - 1):
            total = total + nz[d]
        nsum[...] = total
        for d in range(1, NY):
            remote(nsum, ny.at[d - 1], ny_send, ny_recv, at_y(d)).start()

    todo = [
        (train_norms, 0, 5),
        (meet, 0),
        (train_norms, 5, TRAIN // LANES),
        (fill_norms,),
        (meet, 1),
        (multiply, 0, 0, 2),
        (meet, 2),
        (arrive, 1, 0),
        (multiply, 0, 2, 4),
        (send_z, 0),
        (arrive, 1, 1),
        (multiply, 1, 0, 1),
        (arrive, 1, 2),
        (multiply, 1, 1, 2),
        (relay, 0),
        (arrive, 1, 3),
        (multiply, 1, 2, 3),
        (arrive, 2, 0),
        (send_norms,),
        (multiply, 1, 3, 4),
        (send_z, 1, 2),
        (arrive, 2, 1),
        (multiply, 2, 0, 1),
        (arrive, 2, 2),
        (multiply, 2, 1, 2),
        (arrive, 2, 3),
        (multiply, 2, 2, 3),
        (multiply, 2, 3, 4),
        (send_z, 3),
        (send_y, 0),
        (relay, 1),
        (relay, 2),
        (relay, 3),
        (add_norms,),
        (send_y, 1),
        (send_y, 2),
        (send_y, 3),
    ]
    for what, *how in todo:
        what(*how)

    await_in(ny, ny_recv)
    norms = nsum[...]
    for d in range(NY - 1):
        norms = norms + ny[d]
    nall[...] = norms
    train_norm = jnp.concatenate([norms[NDP + i : NDP + i + 1, :] for i in range(TRAIN // LANES)], axis=1)
    lane = lax.broadcasted_iota(jnp.int32, (8, LANES), 1)
    sub = lax.broadcasted_iota(jnp.int32, (8, LANES), 0)
    rows_norm = jnp.broadcast_to(nall[pl.ds(2 * y + z // 4, 1), :], (8, LANES))
    query_norm = jnp.sum(jnp.where(lane == sub + 8 * (z % 4), rows_norm, 0.0), axis=1, keepdims=True)
    query_scale = lax.rsqrt(query_norm + epsilon)
    train_scale = lax.rsqrt(train_norm + epsilon)

    ahead = (y + NX - x) % NX
    total = zsum[jnp.where(ahead == 0, 0, jnp.where(ahead == 3, 1, ahead + 1))]
    await_in(yin, y_recv)
    for d in range(NY - 1):
        total = total + yin[d]
    out[...] = total * query_scale * train_scale

    await_out(q.at[pl.ds(0, 7)], out_sem)
    await_out(zin, z_send)
    await_out(yin, y_send)
    await_out(qall.at[pl.ds(0, NDP - 1)], qn_send)
    await_out(nz, nz_send)
    await_out(ny, ny_send)


def per_device(train_grads, query_grads):
    f32, bf16 = jnp.float32, jnp.bfloat16
    dma = pltpu.SemaphoreType.DMA
    return pl.pallas_call(
        kernel,
        name="scores",
        out_shape=jax.ShapeDtypeStruct((8, TRAIN), f32),
        in_specs=[pl.BlockSpec(memory_space=pl.ANY)] * 2,
        out_specs=pl.BlockSpec(memory_space=pltpu.VMEM),
        scratch_shapes=[
            pltpu.VMEM((8, 2, HALF, DEPTH), bf16),
            pltpu.VMEM((TRAIN, DEPTH), bf16),
            pltpu.VMEM((32, 8, TRAIN), f32),
            pltpu.VMEM((4, NZ - 1, 8, TRAIN), f32),
            pltpu.VMEM((4, 2, 8, TRAIN), f32),
            pltpu.VMEM((4, 8, TRAIN), f32),
            pltpu.VMEM((NY - 1, 8, TRAIN), f32),
            pltpu.VMEM((TRAIN, LANES), f32),
            pltpu.VMEM((NDP, 1, LANES), f32),
            pltpu.VMEM((16, LANES), f32),
            pltpu.VMEM((NZ - 1, 16, LANES), f32),
            pltpu.VMEM((16, LANES), f32),
            pltpu.VMEM((NY - 1, 16, LANES), f32),
            pltpu.VMEM((16, LANES), f32),
            pltpu.SemaphoreType.REGULAR((6,)),
            dma((2,)),
            dma((TRAIN // LANES,)),
            dma(()),
            dma(()),
            dma((2, NK)),
            dma((2, NK)),
            dma(()),
            dma((4,)),
            dma((4,)),
        ]
        + [dma(())] * 8,
        compiler_params=pltpu.CompilerParams(
            collective_id=0, has_side_effects=True, vmem_limit_bytes=66_700_000
        ),
    )(train_grads, query_grads)


def solution(mesh):
    return jax.shard_map(
        per_device,
        mesh=mesh,
        in_specs=(P("dp", "param"), P("dp", "param")),
        out_specs=P("param", "dp"),
        check_vma=False,
    )
```
